32 devices in a mesh: blk: 4 (over y, core), sub: 2 (over x), kv: 4 (over z).
Axes of the slice: x: 2, y: 2, z: 4, core: 2. Of those that a mesh axis runs over, the one named last changes fastest.
Arguments:
- queries: bfloat16 [4, 8192], P('blk', 'kv'), may hold values from -64 to 64
- cache_keys: bfloat16 [1024, 1024], P(('blk', 'sub'), 'kv'), may hold values from -8 to 8
- cache_values: bfloat16 [1024, 1024], P(('blk', 'sub'), 'kv'), may hold values from -6 to 6
- cache_places: int32 [1024], P(('blk', 'sub')), may hold values from 0 to 1023, as said below
- span_start: int32 [1], replicated, may hold values from 0 to 1020
Outputs:
- attended: bfloat16 [4, 8192], P('blk', 'kv')
- peak_logits: float32 [4, 64], P('blk', 'kv')
The draws below stay inside these ranges and needn't reach their ends.
Inputs may be any that keep to these rules, and one draw needn't show every extreme that they name: `cache_places`: a permutation of 0 to 1023.
All inputs are finite; a program needn't handle non-finite values.
Results may differ from the reference program's by a relative error of at most 0.004.
Values may be sent and summed in bfloat16 or wider, within the bound.
No kernel may reach another device: no remote copies, remote signals or barrier semaphores. Data moves between devices by JAX's collectives and lax.ppermute only.
A program may use at most 64 MiB of HBM per device.

```python
import math
from functools import partial
import jax
import jax.numpy as jnp
from jax import lax

HEADS = 64
KVH = 8
HD = 128
CONTEXT = 1024
SPAN = 4


def joint_draw(key):
    places = jax.random.permutation(jax.random.fold_in(key, 11), CONTEXT).astype(jnp.int32)
    keyset = jnp.clip(1.7 * jax.random.normal(jax.random.fold_in(key, 12), (CONTEXT, KVH * HD), jnp.float32), -8.0, 8.0)
    queryset = jnp.clip(1.8 * jax.random.normal(jax.random.fold_in(key, 13), (SPAN, HEADS * HD), jnp.float32), -10.0, 10.0)
    return (places, keyset, queryset)


def draw_queries(key, part):
    return joint_draw(key)[2].astype(jnp.bfloat16)


def draw_cache_keys(key, part):
    return joint_draw(key)[1].astype(jnp.bfloat16)


def draw_cache_places(key, part):
    return joint_draw(key)[0]


def block_levels(key, extent, shards, least, high):
    def one(axis_at, shards_of):
        heights = jax.random.uniform(jax.random.fold_in(jax.random.fold_in(key, 6), axis_at), (shards_of,), jnp.float32, least / len(shards), high / len(shards))
        return jnp.repeat(jnp.exp(heights), extent[axis_at] // shards_of).reshape((-1,) + (1,) * (len(extent) - axis_at - 1))

    factor_of = one(*shards[0])
    for cut in shards[1:]:
        factor_of = factor_of * one(*cut)
    return factor_of


def bell_draw(own_key, extent, spread, most, shards=(), kind=jnp.bfloat16):
    drawn = jax.random.normal(own_key, extent, jnp.float32) * spread
    if len(shards) > 0:
        drawn = block_levels(own_key, extent, shards, -0.22, 0.18) * drawn
    return jnp.clip(drawn, min=-most, max=most).astype(kind)


def setup_inputs(seed: int = 0) -> dict:
    key_of = jax.random.split(jax.random.key(seed), 6)
    queries = draw_queries(jax.random.fold_in(key_of[5], 71), 0)
    cache_keys = draw_cache_keys(jax.random.fold_in(key_of[5], 71), 0)
    cache_values = bell_draw(key_of[2], (CONTEXT, KVH * HD), 1.0, 6.0, ((0, 8), (1, 4)))
    cache_places = draw_cache_places(jax.random.fold_in(key_of[5], 71), 0)
    span_start = jax.random.randint(key_of[4], (1,), 0, CONTEXT - SPAN + 1).astype(jnp.int32)
    return {"queries": queries, "cache_keys": cache_keys, "cache_values": cache_values, "cache_places": cache_places, "span_start": span_start}


def one_head(queries, cache_keys, cache_values, visible, head_index):
    group_size = HEADS // KVH
    kv_index = head_index // group_size
    query_block = lax.dynamic_slice_in_dim(queries, head_index * HD, HD, 1).astype(jnp.float32)
    key_block = lax.dynamic_slice_in_dim(cache_keys, kv_index * HD, HD, 1).astype(jnp.float32)
    value_block = lax.dynamic_slice_in_dim(cache_values, kv_index * HD, HD, 1).astype(jnp.float32)
    scores = jnp.dot(query_block, key_block.T, precision=lax.Precision.HIGHEST) * (1.0 / math.sqrt(HD))
    shown = visible > 0
    scores = jnp.where(shown, scores, -1e+30)
    peaks = lax.optimization_barrier(jnp.max(scores, axis=1))
    weights = jnp.where(shown, jnp.exp(scores - peaks[:, None]), 0.0).astype(jnp.bfloat16)
    denominator = lax.optimization_barrier(jnp.sum(weights.astype(jnp.float32), axis=1))
    numerator = jnp.dot(weights.astype(jnp.float32), value_block, precision=lax.Precision.HIGHEST)
    return ((numerator / denominator[:, None]).astype(jnp.bfloat16), peaks)

def reference(queries, cache_keys, cache_values, cache_places, span_start):
    offsets = jnp.arange(SPAN, dtype=jnp.int32)
    visible = (cache_places[None, :] <= (span_start[0] + offsets)[:, None]).astype(jnp.int32)
    runner = partial(one_head, queries, cache_keys, cache_values, visible)
    outputs, peaks = lax.map(runner, jnp.arange(HEADS, dtype=jnp.int32))
    attended = jnp.transpose(outputs, (1, 0, 2)).reshape(SPAN, HEADS * HD)
    return (attended, jnp.transpose(peaks, (1, 0)))
```

```python
import functools
import math

import jax
import jax.numpy as jnp
from jax import lax
from jax.experimental import pallas as pl
from jax.experimental.pallas import tpu as pltpu
from jax.sharding import PartitionSpec as P

HD = 128
HIDDEN = -1e30
DIRECT_DEVICES = 16
VMEM_BYTES = 8 * 1024 * 1024


def whole(shape, dtype):
    return jax.ShapeDtypeStruct(shape, dtype)


def params():
    return pltpu.CompilerParams(vmem_limit_bytes=VMEM_BYTES)


def in_vmem(n):
    return [pl.BlockSpec(memory_space=pltpu.VMEM)] * n


def cost(flops):
    return pl.CostEstimate(flops=flops, bytes_accessed=flops // 8, transcendentals=0)


def share_of(query, blocks, shown_rows):
    heads = query.shape[1] // HD
    kv_heads = blocks[0][0].shape[1] // HD
    group = heads // kv_heads
    lane = lax.broadcasted_iota(jnp.int32, (group, HD), 1)
    packed = []
    for j in range(kv_heads):
        first = j * group
        q = jnp.concatenate(
            [query[:, (first + i) * HD : (first + i + 1) * HD] for i in range(group)], axis=0
        )
        scores = [
            jnp.where(
                shown,
                lax.dot_general(
                    q,
                    keys[:, j * HD : (j + 1) * HD],
                    (((1,), (1,)), ((), ())),
                    preferred_element_type=jnp.float32,
                )
                * (1.0 / math.sqrt(HD)),
                HIDDEN,
            )
            for (keys, _), shown in zip(blocks, shown_rows, strict=True)
        ]
        peak = functools.reduce(
            jnp.maximum, [jnp.max(s, axis=1, keepdims=True) for s in scores]
        )
        weights = [
            jnp.where(shown, jnp.exp(s - peak), 0.0).astype(jnp.bfloat16)
            for s, shown in zip(scores, shown_rows, strict=True)
        ]
        denominator = sum(
            jnp.sum(w.astype(jnp.float32), axis=1, keepdims=True) for w in weights
        )
        numerator = sum(
            jnp.dot(w, values[:, j * HD : (j + 1) * HD], preferred_element_type=jnp.float32)
            for w, (_, values) in zip(weights, blocks, strict=True)
        )
        packed.append(
            jnp.concatenate(
                [numerator, jnp.where(lane < HD // 2, peak, denominator)], axis=1
            )
        )
    return jnp.concatenate(packed, axis=0)


def first_kernel(place_ref, query_ref, *refs):
    n = (len(refs) - 2) // 3
    blocks = [(refs[3 * i][...], refs[3 * i + 1][...]) for i in range(n)]
    rows = [refs[3 * i + 2][...] for i in range(n)]
    share_ref, shown_ref = refs[-2:]
    own, other = place_ref[0], place_ref[1]
    share_ref[...] = share_of(query_ref[...], blocks, [r <= own for r in rows])
    for i, r in enumerate(rows):
        shown_ref[i : i + 1] = (r <= other).astype(jnp.int32)


def second_kernel(query_ref, shown_ref, *refs):
    n = (len(refs) - 1) // 2
    blocks = [(refs[2 * i][...], refs[2 * i + 1][...]) for i in range(n)]
    shown = [shown_ref[i : i + 1] > 0 for i in range(n)]
    refs[-1][...] = share_of(query_ref[...], blocks, shown)


def combine_kernel(*refs):
    shares = [r[...] for r in refs[:-2]]
    out_ref, peak_ref = refs[-2:]
    heads = shares[0].shape[0]
    peaks = [s[:, HD : HD + 1] for s in shares]
    peak = functools.reduce(jnp.maximum, peaks)
    scales = [jnp.exp(p - peak) for p in peaks]
    numerator = sum(s[:, :HD] * c for s, c in zip(shares, scales, strict=True))
    denominator = sum(
        s[:, HD + HD // 2 : HD + HD // 2 + 1] * c for s, c in zip(shares, scales, strict=True)
    )
    out = (numerator / denominator).astype(jnp.bfloat16)
    for h in range(heads):
        out_ref[:, h * HD : (h + 1) * HD] = out[h : h + 1]
    row = lax.broadcasted_iota(jnp.int32, (heads, heads), 0)
    column = lax.broadcasted_iota(jnp.int32, (heads, heads), 1)
    peak_ref[...] = jnp.sum(
        jnp.where(row == column, peak, 0.0), axis=0, keepdims=True
    )


def combine(shares, columns):
    heads = shares[0].shape[0]
    return pl.pallas_call(
        combine_kernel,
        out_shape=(whole((1, columns), jnp.bfloat16), whole((1, heads), jnp.float32)),
        in_specs=in_vmem(len(shares)),
        out_specs=tuple(in_vmem(2)),
        compiler_params=params(),
        cost_estimate=cost(1 << 16),
        name="combine",
    )(*shares)


def direct(sizes, queries, cache_keys, cache_values, cache_places, span_start):
    blk, sub = sizes
    columns = queries.shape[1]
    heads = columns // HD
    row_count = cache_keys.shape[0]
    both = ("blk", "sub")

    def swap(value, flip_block, flip_sub):
        pairs = [
            (b * sub + s, (b ^ flip_block) * sub + (s ^ flip_sub))
            for b in range(blk)
            for s in range(sub)
        ]
        return lax.ppermute(value, both, pairs)

    owner = lax.axis_index("blk")
    places = cache_places[None, :]
    other_query = swap(queries, 2, 0)
    far = [swap(x, 1, 0) for x in (cache_keys, cache_values, places)]
    at = span_start[0] + jnp.stack([owner, owner ^ 2]).astype(jnp.int32)
    own_share, shown = pl.pallas_call(
        first_kernel,
        out_shape=(
            whole((heads, 2 * HD), jnp.float32),
            whole((2, row_count), jnp.int32),
        ),
        in_specs=[pl.BlockSpec(memory_space=pltpu.SMEM)] + in_vmem(7),
        out_specs=tuple(in_vmem(2)),
        compiler_params=params(),
        cost_estimate=cost(1 << 22),
        name="own_share",
    )(at, queries, cache_keys, cache_values, places, *far)
    shares = [own_share, swap(own_share, 0, 1)]
    other_share = pl.pallas_call(
        second_kernel,
        out_shape=whole((heads, 2 * HD), jnp.float32),
        in_specs=in_vmem(6),
        out_specs=in_vmem(1)[0],
        compiler_params=params(),
        cost_estimate=cost(1 << 22),
        name="other_share",
    )(other_query, shown, cache_keys, cache_values, *far[:2])
    shares += [swap(other_share, 2, 1), swap(other_share, 2, 0)]
    return combine(shares, columns)


def grouped(queries, cache_keys, cache_values, cache_places, span_start):
    columns = queries.shape[1]
    heads = columns // HD
    kv_heads = cache_keys.shape[1] // HD
    rows_here = queries.shape[0]
    gathered = lax.all_gather(queries, "blk", axis=0, tiled=True)
    count = gathered.shape[0]
    at = span_start[0] + jnp.arange(count, dtype=jnp.int32)
    scores = jnp.einsum(
        "tgjd,rgd->tgjr",
        gathered.reshape(count, kv_heads, heads // kv_heads, HD),
        cache_keys.reshape(-1, kv_heads, HD),
        preferred_element_type=jnp.float32,
    ) * (1.0 / math.sqrt(HD))
    shown = (cache_places[None, :] <= at[:, None])[:, None, None, :]
    scores = jnp.where(shown, scores, HIDDEN)
    peak = jnp.max(scores, axis=3, keepdims=True)
    weights = jnp.where(shown, jnp.exp(scores - peak), 0.0).astype(jnp.bfloat16)
    numerator = jnp.einsum(
        "tgjr,rgd->tgjd",
        weights,
        cache_values.reshape(-1, kv_heads, HD),
        preferred_element_type=jnp.float32,
    )
    denominator = jnp.sum(weights, axis=3, dtype=jnp.float32, keepdims=True)
    shares = jnp.concatenate([numerator, peak, denominator], axis=3)
    shares = shares.reshape(-1, rows_here, heads, HD + 2)
    shares = lax.all_to_all(shares, "blk", 0, 0)
    shares = lax.all_gather(shares, "sub", axis=0, tiled=True)
    peaks = shares[..., HD]
    peak = jnp.max(peaks, axis=0)
    scales = jnp.exp(peaks - peak)
    numerator = jnp.sum(shares[..., :HD] * scales[..., None], axis=0)
    denominator = jnp.sum(shares[..., HD + 1] * scales, axis=0)
    attended = (numerator / denominator[..., None]).astype(jnp.bfloat16)
    return (attended.reshape(rows_here, columns), peak)


def solution(mesh):
    placed = (
        P("blk", "kv"),
        P(("blk", "sub"), "kv"),
        P(("blk", "sub"), "kv"),
        P(("blk", "sub")),
        P(),
    )
    blk, sub = mesh.shape["blk"], mesh.shape["sub"]

    def on_device(queries, *cache):
        if (blk, sub) == (4, 2) and queries.shape[0] == 1:
            return direct((blk, sub), queries, *cache)
        return grouped(queries, *cache)

    return jax.shard_map(
        on_device,
        mesh=mesh,
        in_specs=placed,
        out_specs=(P("blk", "kv"), P("blk", "kv")),
        check_vma=False,
    )
```

```python
import functools
import math

import jax
import jax.numpy as jnp
from jax import lax
from jax.experimental import pallas as pl
from jax.experimental.pallas import tpu as pltpu
from jax.sharding import PartitionSpec as P


HD = 128
HIDDEN = -1e30
VMEM_BYTES = 8 * 1024 * 1024


def whole(shape, dtype):
    return jax.ShapeDtypeStruct(shape, dtype)


def params():
    return pltpu.CompilerParams(vmem_limit_bytes=VMEM_BYTES)


def in_vmem(n):
    return [pl.BlockSpec(memory_space=pltpu.VMEM)] * n


def cost(flops):
    return pl.CostEstimate(flops=flops, bytes_accessed=flops // 8, transcendentals=0)


def share_of(query, blocks, shown_rows):
    heads = query.shape[1] // HD
    kv_heads = blocks[0][0].shape[1] // HD
    group = heads // kv_heads
    lane = lax.broadcasted_iota(jnp.int32, (group, HD), 1)
    packed = []
    for j in range(kv_heads):
        first = j * group
        q = jnp.concatenate(
            [query[:, (first + i) * HD : (first + i + 1) * HD] for i in range(group)], axis=0
        )
        scores = [
            jnp.where(
                shown,
                lax.dot_general(
                    q,
                    keys[:, j * HD : (j + 1) * HD],
                    (((1,), (1,)), ((), ())),
                    preferred_element_type=jnp.float32,
                )
                * (1.0 / math.sqrt(HD)),
                HIDDEN,
            )
            for (keys, _), shown in zip(blocks, shown_rows, strict=True)
        ]
        peak = functools.reduce(
            jnp.maximum, [jnp.max(s, axis=1, keepdims=True) for s in scores]
        )
        weights = [
            jnp.where(shown, jnp.exp(s - peak), 0.0).astype(jnp.bfloat16)
            for s, shown in zip(scores, shown_rows, strict=True)
        ]
        denominator = sum(
            jnp.sum(w.astype(jnp.float32), axis=1, keepdims=True) for w in weights
        )
        numerator = sum(
            jnp.dot(w, values[:, j * HD : (j + 1) * HD], preferred_element_type=jnp.float32)
            for w, (_, values) in zip(weights, blocks, strict=True)
        )
        packed.append(
            jnp.concatenate(
                [numerator, jnp.where(lane < HD // 2, peak, denominator)], axis=1
            )
        )
    return jnp.concatenate(packed, axis=0)


def clock_kernel(owners, start_ref, clock_ref):
    for i, owner in enumerate(owners):
        at = start_ref[0] + owner(lax.axis_index("blk"))
        clock_ref[i : i + 1] = jnp.full((1, clock_ref.shape[1]), at, jnp.int32)


def share_kernel(row, clock_ref, query_ref, *refs):
    n = (len(refs) - 1) // 3
    blocks = [(refs[3 * i][...], refs[3 * i + 1][...]) for i in range(n)]
    clock = clock_ref[row : row + 1]
    shown = [refs[3 * i + 2][...] <= clock for i in range(n)]
    refs[-1][...] = share_of(query_ref[...], blocks, shown)


def combine_kernel(*refs):
    shares = [r[...] for r in refs[:-2]]
    out_ref, peak_ref = refs[-2:]
    heads = shares[0].shape[0]
    peaks = [s[:, HD : HD + 1] for s in shares]
    peak = functools.reduce(jnp.maximum, peaks)
    scales = [jnp.exp(p - peak) for p in peaks]
    numerator = sum(s[:, :HD] * c for s, c in zip(shares, scales, strict=True))
    denominator = sum(
        s[:, HD + HD // 2 : HD + HD // 2 + 1] * c for s, c in zip(shares, scales, strict=True)
    )
    out = (numerator / denominator).astype(jnp.bfloat16)
    for h in range(heads):
        out_ref[:, h * HD : (h + 1) * HD] = out[h : h + 1]
    row = lax.broadcasted_iota(jnp.int32, (heads, heads), 0)
    column = lax.broadcasted_iota(jnp.int32, (heads, heads), 1)
    peak_ref[...] = jnp.sum(
        jnp.where(row == column, peak, 0.0), axis=0, keepdims=True
    )


def combine(shares, columns):
    heads = shares[0].shape[0]
    return pl.pallas_call(
        combine_kernel,
        out_shape=(whole((1, columns), jnp.bfloat16), whole((1, heads), jnp.float32)),
        in_specs=in_vmem(len(shares)),
        out_specs=tuple(in_vmem(2)),
        compiler_params=params(),
        cost_estimate=cost(1 << 16),
        name="combine",
    )(*shares)


def direct(sizes, queries, cache_keys, cache_values, cache_places, span_start):
    blk, sub = sizes
    columns = queries.shape[1]
    heads = columns // HD
    row_count = cache_keys.shape[0]
    both = ("blk", "sub")

    def swap(value, flip_block, flip_sub):
        pairs = [
            (b * sub + s, (b ^ flip_block) * sub + (s ^ flip_sub))
            for b in range(blk)
            for s in range(sub)
        ]
        return lax.ppermute(value, both, pairs)

    def share(row, query):
        return pl.pallas_call(
            functools.partial(share_kernel, row),
            out_shape=whole((heads, 2 * HD), jnp.float32),
            in_specs=in_vmem(8),
            out_specs=in_vmem(1)[0],
            compiler_params=params(),
            cost_estimate=cost(1 << 22),
        )(clock, query, cache_keys, cache_values, places, *far)

    places = cache_places[None, :]
    other_query = swap(queries, 3, 0)
    far = [swap(cache_keys, 1, 0), swap(cache_values, 1, 0), swap(places, 1, 0)]
    clock = pl.pallas_call(
        functools.partial(clock_kernel, (lambda b: b, lambda b: b ^ 3)),
        out_shape=whole((2, row_count), jnp.int32),
        in_specs=[pl.BlockSpec(memory_space=pltpu.SMEM)],
        out_specs=in_vmem(1)[0],
        compiler_params=params(),
        cost_estimate=pl.CostEstimate(flops=1 << 27, bytes_accessed=4096, transcendentals=0),
        name="clock",
    )(span_start)
    own_share = share(0, queries)
    across = swap(own_share, 0, 1)
    other_share = share(1, other_query)
    shares = [own_share, across, swap(other_share, 3, 1), swap(other_share, 3, 0)]
    return combine(shares, columns)


def grouped(queries, cache_keys, cache_values, cache_places, span_start):
    columns = queries.shape[1]
    heads = columns // HD
    kv_heads = cache_keys.shape[1] // HD
    rows_here = queries.shape[0]
    gathered = lax.all_gather(queries, "blk", axis=0, tiled=True)
    count = gathered.shape[0]
    at = span_start[0] + jnp.arange(count, dtype=jnp.int32)
    scores = jnp.einsum(
        "tgjd,rgd->tgjr",
        gathered.reshape(count, kv_heads, heads // kv_heads, HD),
        cache_keys.reshape(-1, kv_heads, HD),
        preferred_element_type=jnp.float32,
    ) * (1.0 / math.sqrt(HD))
    shown = (cache_places[None, :] <= at[:, None])[:, None, None, :]
    scores = jnp.where(shown, scores, HIDDEN)
    peak = jnp.max(scores, axis=3, keepdims=True)
    weights = jnp.where(shown, jnp.exp(scores - peak), 0.0).astype(jnp.bfloat16)
    numerator = jnp.einsum(
        "tgjr,rgd->tgjd",
        weights,
        cache_values.reshape(-1, kv_heads, HD),
        preferred_element_type=jnp.float32,
    )
    denominator = jnp.sum(weights, axis=3, dtype=jnp.float32, keepdims=True)
    shares = jnp.concatenate([numerator, peak, denominator], axis=3)
    shares = shares.reshape(-1, rows_here, heads, HD + 2)
    shares = lax.all_to_all(shares, "blk", 0, 0)
    shares = lax.all_gather(shares, "sub", axis=0, tiled=True)
    peaks = shares[..., HD]
    peak = jnp.max(peaks, axis=0)
    scales = jnp.exp(peaks - peak)
    numerator = jnp.sum(shares[..., :HD] * scales[..., None], axis=0)
    denominator = jnp.sum(shares[..., HD + 1] * scales, axis=0)
    attended = (numerator / denominator[..., None]).astype(jnp.bfloat16)
    return (attended.reshape(rows_here, columns), peak)


def solution(mesh):
    placed = (
        P("blk", "kv"),
        P(("blk", "sub"), "kv"),
        P(("blk", "sub"), "kv"),
        P(("blk", "sub")),
        P(),
    )
    blk, sub = mesh.shape["blk"], mesh.shape["sub"]
    is_direct = (blk, sub) == (4, 2) and mesh.size <= 32

    def on_device(queries, *cache):
        if is_direct and queries.shape[0] == 1:
            return direct((blk, sub), queries, *cache)
        return grouped(queries, *cache)

    return jax.shard_map(
        on_device,
        mesh=mesh,
        in_specs=placed,
        out_specs=(P("blk", "kv"), P("blk", "kv")),
        check_vma=False,
    )
```

```python
import functools
import math

import jax
import jax.numpy as jnp
from jax import lax
from jax.experimental import pallas as pl
from jax.experimental.pallas import tpu as pltpu
from jax.sharding import PartitionSpec as P


HD = 128
HIDDEN = -1e30
VMEM_BYTES = 8 * 1024 * 1024


def whole(shape, dtype):
    return jax.ShapeDtypeStruct(shape, dtype)


def params():
    return pltpu.CompilerParams(vmem_limit_bytes=VMEM_BYTES)


def in_vmem(n):
    return [pl.BlockSpec(memory_space=pltpu.VMEM)] * n


def cost(flops):
    return pl.CostEstimate(flops=flops, bytes_accessed=flops // 8, transcendentals=0)


def share_of(query, blocks, shown_rows):
    heads = query.shape[1] // HD
    kv_heads = blocks[0][0].shape[1] // HD
    group = heads // kv_heads
    lane = lax.broadcasted_iota(jnp.int32, (group, HD), 1)
    packed = []
    for j in range(kv_heads):
        first = j * group
        q = jnp.concatenate(
            [query[:, (first + i) * HD : (first + i + 1) * HD] for i in range(group)], axis=0
        )
        scores = [
            jnp.where(
                shown,
                lax.dot_general(
                    q,
                    keys[:, j * HD : (j + 1) * HD],
                    (((1,), (1,)), ((), ())),
                    preferred_element_type=jnp.float32,
                )
                * (1.0 / math.sqrt(HD)),
                HIDDEN,
            )
            for (keys, _), shown in zip(blocks, shown_rows, strict=True)
        ]
        peak = functools.reduce(
            jnp.maximum, [jnp.max(s, axis=1, keepdims=True) for s in scores]
        )
        weights = [
            jnp.where(shown, jnp.exp(s - peak), 0.0).astype(jnp.bfloat16)
            for s, shown in zip(scores, shown_rows, strict=True)
        ]
        denominator = sum(
            jnp.sum(w.astype(jnp.float32), axis=1, keepdims=True) for w in weights
        )
        numerator = sum(
            jnp.dot(w, values[:, j * HD : (j + 1) * HD], preferred_element_type=jnp.float32)
            for w, (_, values) in zip(weights, blocks, strict=True)
        )
        packed.append(
            jnp.concatenate(
                [numerator, jnp.where(lane < HD // 2, peak, denominator)], axis=1
            )
        )
    return jnp.concatenate(packed, axis=0)


def tokens_kernel(owners, tokens_ref):
    for i, owner in enumerate(owners):
        at = owner(lax.axis_index("blk"))
        tokens_ref[i : i + 1] = jnp.full((1, tokens_ref.shape[1]), at, jnp.int32)


def clock_kernel(start_ref, tokens_ref, clock_ref):
    clock_ref[...] = tokens_ref[...] + start_ref[0]


def share_kernel(row, clock_ref, query_ref, *refs):
    n = (len(refs) - 1) // 3
    blocks = [(refs[3 * i][...], refs[3 * i + 1][...]) for i in range(n)]
    clock = clock_ref[row : row + 1]
    shown = [refs[3 * i + 2][...] <= clock for i in range(n)]
    refs[-1][...] = share_of(query_ref[...], blocks, shown)


def combine_kernel(*refs):
    shares = [r[...] for r in refs[:-2]]
    out_ref, peak_ref = refs[-2:]
    heads = shares[0].shape[0]
    peaks = [s[:, HD : HD + 1] for s in shares]
    peak = functools.reduce(jnp.maximum, peaks)
    scales = [jnp.exp(p - peak) for p in peaks]
    numerator = sum(s[:, :HD] * c for s, c in zip(shares, scales, strict=True))
    denominator = sum(
        s[:, HD + HD // 2 : HD + HD // 2 + 1] * c for s, c in zip(shares, scales, strict=True)
    )
    out = (numerator / denominator).astype(jnp.bfloat16)
    for h in range(heads):
        out_ref[:, h * HD : (h + 1) * HD] = out[h : h + 1]
    row = lax.broadcasted_iota(jnp.int32, (heads, heads), 0)
    column = lax.broadcasted_iota(jnp.int32, (heads, heads), 1)
    peak_ref[...] = jnp.sum(
        jnp.where(row == column, peak, 0.0), axis=0, keepdims=True
    )


def combine(shares, columns):
    heads = shares[0].shape[0]
    return pl.pallas_call(
        combine_kernel,
        out_shape=(whole((1, columns), jnp.bfloat16), whole((1, heads), jnp.float32)),
        in_specs=in_vmem(len(shares)),
        out_specs=tuple(in_vmem(2)),
        compiler_params=params(),
        cost_estimate=cost(1 << 16),
        name="combine",
    )(*shares)


def direct(sizes, queries, cache_keys, cache_values, cache_places, span_start):
    blk, sub = sizes
    columns = queries.shape[1]
    heads = columns // HD
    row_count = cache_keys.shape[0]
    both = ("blk", "sub")

    def swap(value, flip_block, flip_sub):
        pairs = [
            (b * sub + s, (b ^ flip_block) * sub + (s ^ flip_sub))
            for b in range(blk)
            for s in range(sub)
        ]
        return lax.ppermute(value, both, pairs)

    def share(row, query):
        return pl.pallas_call(
            functools.partial(share_kernel, row),
            out_shape=whole((heads, 2 * HD), jnp.float32),
            in_specs=in_vmem(8),
            out_specs=in_vmem(1)[0],
            compiler_params=params(),
            cost_estimate=cost(1 << 22),
        )(clock, query, cache_keys, cache_values, places, *far)

    places = cache_places[None, :]
    other_query = swap(queries, 3, 0)
    far = [swap(cache_keys, 1, 0), swap(cache_values, 1, 0), swap(places, 1, 0)]
    tokens = pl.pallas_call(
        functools.partial(tokens_kernel, (lambda b: b, lambda b: b ^ 3)),
        out_shape=whole((2, row_count), jnp.int32),
        out_specs=in_vmem(1)[0],
        compiler_params=params(),
        cost_estimate=pl.CostEstimate(
            flops=1 << 27, bytes_accessed=4096, transcendentals=0
        ),
        name="tokens",
    )()
    clock = pl.pallas_call(
        clock_kernel,
        out_shape=whole((2, row_count), jnp.int32),
        in_specs=[pl.BlockSpec(memory_space=pltpu.SMEM)] + in_vmem(1),
        out_specs=in_vmem(1)[0],
        compiler_params=params(),
        cost_estimate=cost(1 << 12),
        name="clock",
    )(span_start, tokens)
    own_share = share(0, queries)
    across = swap(own_share, 0, 1)
    other_share = share(1, other_query)
    shares = [own_share, across, swap(other_share, 3, 1), swap(other_share, 3, 0)]
    return combine(shares, columns)


def grouped(queries, cache_keys, cache_values, cache_places, span_start):
    columns = queries.shape[1]
    heads = columns // HD
    kv_heads = cache_keys.shape[1] // HD
    rows_here = queries.shape[0]
    gathered = lax.all_gather(queries, "blk", axis=0, tiled=True)
    count = gathered.shape[0]
    at = span_start[0] + jnp.arange(count, dtype=jnp.int32)
    scores = jnp.einsum(
        "tgjd,rgd->tgjr",
        gathered.reshape(count, kv_heads, heads // kv_heads, HD),
        cache_keys.reshape(-1, kv_heads, HD),
        preferred_element_type=jnp.float32,
    ) * (1.0 / math.sqrt(HD))
    shown = (cache_places[None, :] <= at[:, None])[:, None, None, :]
    scores = jnp.where(shown, scores, HIDDEN)
    peak = jnp.max(scores, axis=3, keepdims=True)
    weights = jnp.where(shown, jnp.exp(scores - peak), 0.0).astype(jnp.bfloat16)
    numerator = jnp.einsum(
        "tgjr,rgd->tgjd",
        weights,
        cache_values.reshape(-1, kv_heads, HD),
        preferred_element_type=jnp.float32,
    )
    denominator = jnp.sum(weights, axis=3, dtype=jnp.float32, keepdims=True)
    shares = jnp.concatenate([numerator, peak, denominator], axis=3)
    shares = shares.reshape(-1, rows_here, heads, HD + 2)
    shares = lax.all_to_all(shares, "blk", 0, 0)
    shares = lax.all_gather(shares, "sub", axis=0, tiled=True)
    peaks = shares[..., HD]
    peak = jnp.max(peaks, axis=0)
    scales = jnp.exp(peaks - peak)
    numerator = jnp.sum(shares[..., :HD] * scales[..., None], axis=0)
    denominator = jnp.sum(shares[..., HD + 1] * scales, axis=0)
    attended = (numerator / denominator[..., None]).astype(jnp.bfloat16)
    return (attended.reshape(rows_here, columns), peak)


def solution(mesh):
    placed = (
        P("blk", "kv"),
        P(("blk", "sub"), "kv"),
        P(("blk", "sub"), "kv"),
        P(("blk", "sub")),
        P(),
    )
    blk, sub = mesh.shape["blk"], mesh.shape["sub"]
    is_direct = (blk, sub) == (4, 2) and mesh.size <= 32

    def on_device(queries, *cache):
        if is_direct and queries.shape[0] == 1:
            return direct((blk, sub), queries, *cache)
        return grouped(queries, *cache)

    return jax.shard_map(
        on_device,
        mesh=mesh,
        in_specs=placed,
        out_specs=(P("blk", "kv"), P("blk", "kv")),
        check_vma=False,
    )
```

```python
import functools
import math

import jax
import jax.numpy as jnp
from jax import lax
from jax.experimental import pallas as pl
from jax.experimental.pallas import tpu as pltpu
from jax.sharding import PartitionSpec as P


HD = 128
HIDDEN = -1e30
VMEM_BYTES = 8 * 1024 * 1024


def whole(shape, dtype):
    return jax.ShapeDtypeStruct(shape, dtype)


def params():
    return pltpu.CompilerParams(vmem_limit_bytes=VMEM_BYTES)


def in_vmem(n):
    return [pl.BlockSpec(memory_space=pltpu.VMEM)] * n


def cost(flops):
    return pl.CostEstimate(flops=flops, bytes_accessed=flops // 8, transcendentals=0)


def share_of(query, blocks, shown_rows):
    heads = query.shape[1] // HD
    kv_heads = blocks[0][0].shape[1] // HD
    group = heads // kv_heads
    rows = jnp.concatenate([query[:, i * HD : (i + 1) * HD] for i in range(heads)], axis=0)
    kv_of = lax.broadcasted_iota(jnp.int32, (heads, HD), 0) // group
    lane = lax.broadcasted_iota(jnp.int32, (heads, HD), 1)
    spread = jnp.concatenate(
        [jnp.where(kv_of == j, rows, jnp.zeros_like(rows)) for j in range(kv_heads)], axis=1
    )
    scores = [
        jnp.where(
            shown,
            lax.dot_general(
                spread, keys, (((1,), (1,)), ((), ())), preferred_element_type=jnp.float32
            )
            * (1.0 / math.sqrt(HD)),
            HIDDEN,
        )
        for (keys, _), shown in zip(blocks, shown_rows, strict=True)
    ]
    peak = functools.reduce(jnp.maximum, [jnp.max(s, axis=1, keepdims=True) for s in scores])
    weights = [
        jnp.where(shown, jnp.exp(s - peak), 0.0).astype(jnp.bfloat16)
        for s, shown in zip(scores, shown_rows, strict=True)
    ]
    denominator = sum(jnp.sum(w.astype(jnp.float32), axis=1, keepdims=True) for w in weights)
    wide = sum(
        jnp.dot(w, values, preferred_element_type=jnp.float32)
        for w, (_, values) in zip(weights, blocks, strict=True)
    )
    numerator = wide[:, :HD]
    for j in range(1, kv_heads):
        numerator = jnp.where(kv_of == j, wide[:, j * HD : (j + 1) * HD], numerator)
    return jnp.concatenate([numerator, jnp.where(lane < HD // 2, peak, denominator)], axis=1)


def tokens_kernel(owners, tokens_ref):
    for i, owner in enumerate(owners):
        at = owner(lax.axis_index("blk"))
        tokens_ref[i : i + 1] = jnp.full((1, tokens_ref.shape[1]), at, jnp.int32)


def clock_kernel(start_ref, tokens_ref, clock_ref):
    clock_ref[...] = tokens_ref[...] + start_ref[0]


def share_kernel(row, clock_ref, query_ref, *refs):
    n = (len(refs) - 1) // 3
    blocks = [(refs[3 * i][...], refs[3 * i + 1][...]) for i in range(n)]
    clock = clock_ref[row : row + 1]
    shown = [refs[3 * i + 2][...] <= clock for i in range(n)]
    refs[-1][...] = share_of(query_ref[...], blocks, shown)


def combine_kernel(*refs):
    shares = [r[...] for r in refs[:-2]]
    out_ref, peak_ref = refs[-2:]
    heads = shares[0].shape[0]
    peaks = [s[:, HD : HD + 1] for s in shares]
    peak = functools.reduce(jnp.maximum, peaks)
    scales = [jnp.exp(p - peak) for p in peaks]
    numerator = sum(s[:, :HD] * c for s, c in zip(shares, scales, strict=True))
    denominator = sum(
        s[:, HD + HD // 2 : HD + HD // 2 + 1] * c for s, c in zip(shares, scales, strict=True)
    )
    out = (numerator / denominator).astype(jnp.bfloat16)
    for h in range(heads):
        out_ref[:, h * HD : (h + 1) * HD] = out[h : h + 1]
    row = lax.broadcasted_iota(jnp.int32, (heads, heads), 0)
    column = lax.broadcasted_iota(jnp.int32, (heads, heads), 1)
    peak_ref[...] = jnp.sum(
        jnp.where(row == column, peak, 0.0), axis=0, keepdims=True
    )


def combine(shares, columns):
    heads = shares[0].shape[0]
    return pl.pallas_call(
        combine_kernel,
        out_shape=(whole((1, columns), jnp.bfloat16), whole((1, heads), jnp.float32)),
        in_specs=in_vmem(len(shares)),
        out_specs=tuple(in_vmem(2)),
        compiler_params=params(),
        cost_estimate=cost(1 << 16),
        name="combine",
    )(*shares)


def direct(sizes, queries, cache_keys, cache_values, cache_places, span_start):
    blk, sub = sizes
    columns = queries.shape[1]
    heads = columns // HD
    row_count = cache_keys.shape[0]
    both = ("blk", "sub")

    def swap(value, flip_block, flip_sub):
        pairs = [
            (b * sub + s, (b ^ flip_block) * sub + (s ^ flip_sub))
            for b in range(blk)
            for s in range(sub)
        ]
        return lax.ppermute(value, both, pairs)

    def share(row, query):
        return pl.pallas_call(
            functools.partial(share_kernel, row),
            out_shape=whole((heads, 2 * HD), jnp.float32),
            in_specs=in_vmem(8),
            out_specs=in_vmem(1)[0],
            compiler_params=params(),
            cost_estimate=cost(1 << 22),
        )(clock, query, cache_keys, cache_values, places, *far)

    places = cache_places[None, :]
    other_query = swap(queries, 3, 0)
    far = [swap(cache_keys, 1, 0), swap(cache_values, 1, 0), swap(places, 1, 0)]
    tokens = pl.pallas_call(
        functools.partial(tokens_kernel, (lambda b: b, lambda b: b ^ 3)),
        out_shape=whole((2, row_count), jnp.int32),
        out_specs=in_vmem(1)[0],
        compiler_params=params(),
        cost_estimate=pl.CostEstimate(
            flops=1 << 27, bytes_accessed=4096, transcendentals=0
        ),
        name="tokens",
    )()
    clock = pl.pallas_call(
        clock_kernel,
        out_shape=whole((2, row_count), jnp.int32),
        in_specs=[pl.BlockSpec(memory_space=pltpu.SMEM)] + in_vmem(1),
        out_specs=in_vmem(1)[0],
        compiler_params=params(),
        cost_estimate=cost(1 << 12),
        name="clock",
    )(span_start, tokens)
    own_share = share(0, queries)
    across = swap(own_share, 0, 1)
    other_share = share(1, other_query)
    shares = [own_share, across, swap(other_share, 3, 1), swap(other_share, 3, 0)]
    return combine(shares, columns)


def grouped(queries, cache_keys, cache_values, cache_places, span_start):
    columns = queries.shape[1]
    heads = columns // HD
    kv_heads = cache_keys.shape[1] // HD
    rows_here = queries.shape[0]
    gathered = lax.all_gather(queries, "blk", axis=0, tiled=True)
    count = gathered.shape[0]
    at = span_start[0] + jnp.arange(count, dtype=jnp.int32)
    scores = jnp.einsum(
        "tgjd,rgd->tgjr",
        gathered.reshape(count, kv_heads, heads // kv_heads, HD),
        cache_keys.reshape(-1, kv_heads, HD),
        preferred_element_type=jnp.float32,
    ) * (1.0 / math.sqrt(HD))
    shown = (cache_places[None, :] <= at[:, None])[:, None, None, :]
    scores = jnp.where(shown, scores, HIDDEN)
    peak = jnp.max(scores, axis=3, keepdims=True)
    weights = jnp.where(shown, jnp.exp(scores - peak), 0.0).astype(jnp.bfloat16)
    numerator = jnp.einsum(
        "tgjr,rgd->tgjd",
        weights,
        cache_values.reshape(-1, kv_heads, HD),
        preferred_element_type=jnp.float32,
    )
    denominator = jnp.sum(weights, axis=3, dtype=jnp.float32, keepdims=True)
    shares = jnp.concatenate([numerator, peak, denominator], axis=3)
    shares = shares.reshape(-1, rows_here, heads, HD + 2)
    shares = lax.all_to_all(shares, "blk", 0, 0)
    shares = lax.all_gather(shares, "sub", axis=0, tiled=True)
    peaks = shares[..., HD]
    peak = jnp.max(peaks, axis=0)
    scales = jnp.exp(peaks - peak)
    numerator = jnp.sum(shares[..., :HD] * scales[..., None], axis=0)
    denominator = jnp.sum(shares[..., HD + 1] * scales, axis=0)
    attended = (numerator / denominator[..., None]).astype(jnp.bfloat16)
    return (attended.reshape(rows_here, columns), peak)


def solution(mesh):
    placed = (
        P("blk", "kv"),
        P(("blk", "sub"), "kv"),
        P(("blk", "sub"), "kv"),
        P(("blk", "sub")),
        P(),
    )
    blk, sub = mesh.shape["blk"], mesh.shape["sub"]
    is_direct = (blk, sub) == (4, 2) and mesh.size <= 32

    def on_device(queries, *cache):
        if is_direct and queries.shape[0] == 1:
            return direct((blk, sub), queries, *cache)
        return grouped(queries, *cache)

    return jax.shard_map(
        on_device,
        mesh=mesh,
        in_specs=placed,
        out_specs=(P("blk", "kv"), P("blk", "kv")),
        check_vma=False,
    )
```

```python
import functools
import math

import jax
import jax.numpy as jnp
from jax import lax
from jax.experimental import pallas as pl
from jax.experimental.pallas import tpu as pltpu
from jax.sharding import PartitionSpec as P


HD = 128
HIDDEN = -1e30
DIGIT_ROWS = 16
STRETCH = 16
VMEM_BYTES = 8 * 1024 * 1024


def whole(shape, dtype):
    return jax.ShapeDtypeStruct(shape, dtype)


def params():
    return pltpu.CompilerParams(vmem_limit_bytes=VMEM_BYTES)


def in_vmem(n):
    return [pl.BlockSpec(memory_space=pltpu.VMEM)] * n


def cost(flops):
    return pl.CostEstimate(flops=flops, bytes_accessed=flops // 8, transcendentals=0)


def terms_of(column):
    terms = []
    for _ in range(3):
        term = column.astype(jnp.bfloat16).astype(jnp.float32)
        terms.append(term)
        column = column - term
    return terms


def share_of(query, blocks, shown_rows):
    heads = query.shape[1] // HD
    kv_heads = blocks[0][0].shape[1] // HD
    group = heads // kv_heads
    rows = jnp.concatenate([query[:, i * HD : (i + 1) * HD] for i in range(heads)], axis=0)
    kv_of = lax.broadcasted_iota(jnp.int32, (heads, HD), 0) // group
    lane = lax.broadcasted_iota(jnp.int32, (heads, HD), 1)
    spread = jnp.concatenate(
        [jnp.where(kv_of == j, rows, jnp.zeros_like(rows)) for j in range(kv_heads)], axis=1
    )
    scores = [
        jnp.where(
            shown,
            lax.dot_general(
                spread, keys, (((1,), (1,)), ((), ())), preferred_element_type=jnp.float32
            )
            * (1.0 / math.sqrt(HD)),
            HIDDEN,
        )
        for (keys, _), shown in zip(blocks, shown_rows, strict=True)
    ]
    peak = functools.reduce(jnp.maximum, [jnp.max(s, axis=1, keepdims=True) for s in scores])
    weights = [
        jnp.where(shown, jnp.exp(s - peak), 0.0).astype(jnp.bfloat16)
        for s, shown in zip(scores, shown_rows, strict=True)
    ]
    denominator = sum(jnp.sum(w.astype(jnp.float32), axis=1, keepdims=True) for w in weights)
    wide = sum(
        jnp.dot(w, values, preferred_element_type=jnp.float32)
        for w, (_, values) in zip(weights, blocks, strict=True)
    )
    numerator = wide[:, :HD]
    for j in range(1, kv_heads):
        numerator = jnp.where(kv_of == j, wide[:, j * HD : (j + 1) * HD], numerator)
    terms = [*terms_of(peak), *terms_of(denominator)]
    stats = terms[-1]
    for i in range(len(terms) - 2, -1, -1):
        stats = jnp.where(lane < (i + 1) * STRETCH, terms[i], stats)
    return jnp.concatenate([numerator, stats], axis=1).astype(jnp.bfloat16)


def tokens_kernel(owners, tokens_ref):
    for i, owner in enumerate(owners):
        at = owner(lax.axis_index("blk"))
        tokens_ref[i : i + 1] = jnp.full((1, tokens_ref.shape[1]), at, jnp.int32)


def clock_kernel(start_ref, tokens_ref, clock_ref):
    clock_ref[...] = tokens_ref[...] + start_ref[0]


def pack_kernel(keys_ref, values_ref, places_ref, packed_ref):
    rows, columns = keys_ref.shape
    packed_ref[:rows] = keys_ref[...]
    packed_ref[rows : 2 * rows] = values_ref[...]
    places = places_ref[...].reshape(1, rows)
    digit = lax.broadcasted_iota(jnp.int32, (DIGIT_ROWS, rows), 0)
    digits = jnp.where(digit == 0, places >> 8, jnp.where(digit == 1, places & 255, 0))
    packed_ref[2 * rows :, :rows] = digits.astype(jnp.float32).astype(jnp.bfloat16)
    packed_ref[2 * rows :, rows:] = jnp.zeros((DIGIT_ROWS, columns - rows), jnp.bfloat16)


def share_kernel(row, clock_ref, query_ref, *refs):
    clock = clock_ref[row : row + 1].astype(jnp.float32)
    rows = (refs[0].shape[0] - DIGIT_ROWS) // 2
    blocks, shown = [], []
    for ref in refs[:-1]:
        blocks.append((ref[:rows], ref[rows : 2 * rows]))
        digits = ref[2 * rows :, :rows].astype(jnp.float32)
        shown.append(digits[:1] * 256.0 + digits[1:2] <= clock)
    refs[-1][...] = share_of(query_ref[...], blocks, shown)


def stat_of(share, first):
    at = HD + first * STRETCH
    terms = [share[:, at + i * STRETCH : at + i * STRETCH + 1] for i in range(3)]
    return terms[0] + terms[1] + terms[2]


def combine_kernel(*refs):
    shares = [r[...].astype(jnp.float32) for r in refs[:-2]]
    out_ref, peak_ref = refs[-2:]
    heads = shares[0].shape[0]
    peaks = [stat_of(s, 0) for s in shares]
    peak = functools.reduce(jnp.maximum, peaks)
    scales = [jnp.exp(p - peak) for p in peaks]
    numerator = sum(s[:, :HD] * c for s, c in zip(shares, scales, strict=True))
    denominator = sum(stat_of(s, 3) * c for s, c in zip(shares, scales, strict=True))
    out = (numerator / denominator).astype(jnp.bfloat16)
    for h in range(heads):
        out_ref[:, h * HD : (h + 1) * HD] = out[h : h + 1]
    row = lax.broadcasted_iota(jnp.int32, (heads, heads), 0)
    column = lax.broadcasted_iota(jnp.int32, (heads, heads), 1)
    peak_ref[...] = jnp.sum(
        jnp.where(row == column, peak, 0.0), axis=0, keepdims=True
    )


def combine(shares, columns):
    heads = shares[0].shape[0]
    return pl.pallas_call(
        combine_kernel,
        out_shape=(whole((1, columns), jnp.bfloat16), whole((1, heads), jnp.float32)),
        in_specs=in_vmem(len(shares)),
        out_specs=tuple(in_vmem(2)),
        compiler_params=params(),
        cost_estimate=cost(1 << 16),
        name="combine",
    )(*shares)


def direct(sizes, queries, cache_keys, cache_values, cache_places, span_start):
    blk, sub = sizes
    columns = queries.shape[1]
    heads = columns // HD
    row_count = cache_keys.shape[0]
    both = ("blk", "sub")

    def swap(value, flip_block, flip_sub):
        pairs = [
            (b * sub + s, (b ^ flip_block) * sub + (s ^ flip_sub))
            for b in range(blk)
            for s in range(sub)
        ]
        return lax.ppermute(value, both, pairs)

    def share(row, query):
        return pl.pallas_call(
            functools.partial(share_kernel, row),
            out_shape=whole((heads, 2 * HD), jnp.bfloat16),
            in_specs=in_vmem(4),
            out_specs=in_vmem(1)[0],
            compiler_params=params(),
            cost_estimate=cost(1 << 22),
        )(clock, query, mine, theirs)

    other_query = swap(queries, 3, 0)
    mine = pl.pallas_call(
        pack_kernel,
        out_shape=whole((2 * row_count + DIGIT_ROWS, cache_keys.shape[1]), jnp.bfloat16),
        in_specs=in_vmem(3),
        out_specs=in_vmem(1)[0],
        compiler_params=params(),
        cost_estimate=cost(1 << 12),
        name="pack",
    )(cache_keys, cache_values, cache_places)
    theirs = swap(mine, 1, 0)
    tokens = pl.pallas_call(
        functools.partial(tokens_kernel, (lambda b: b, lambda b: b ^ 3)),
        out_shape=whole((2, row_count), jnp.int32),
        out_specs=in_vmem(1)[0],
        compiler_params=params(),
        cost_estimate=pl.CostEstimate(
            flops=1 << 27, bytes_accessed=4096, transcendentals=0
        ),
        name="tokens",
    )()
    clock = pl.pallas_call(
        clock_kernel,
        out_shape=whole((2, row_count), jnp.int32),
        in_specs=[pl.BlockSpec(memory_space=pltpu.SMEM)] + in_vmem(1),
        out_specs=in_vmem(1)[0],
        compiler_params=params(),
        cost_estimate=cost(1 << 12),
        name="clock",
    )(span_start, tokens)
    own_share = share(0, queries)
    across = swap(own_share, 0, 1)
    other_share = share(1, other_query)
    shares = [own_share, across, swap(other_share, 3, 1), swap(other_share, 3, 0)]
    return combine(shares, columns)


def grouped(queries, cache_keys, cache_values, cache_places, span_start):
    columns = queries.shape[1]
    heads = columns // HD
    kv_heads = cache_keys.shape[1] // HD
    rows_here = queries.shape[0]
    gathered = lax.all_gather(queries, "blk", axis=0, tiled=True)
    count = gathered.shape[0]
    at = span_start[0] + jnp.arange(count, dtype=jnp.int32)
    scores = jnp.einsum(
        "tgjd,rgd->tgjr",
        gathered.reshape(count, kv_heads, heads // kv_heads, HD),
        cache_keys.reshape(-1, kv_heads, HD),
        preferred_element_type=jnp.float32,
    ) * (1.0 / math.sqrt(HD))
    shown = (cache_places[None, :] <= at[:, None])[:, None, None, :]
    scores = jnp.where(shown, scores, HIDDEN)
    peak = jnp.max(scores, axis=3, keepdims=True)
    weights = jnp.where(shown, jnp.exp(scores - peak), 0.0).astype(jnp.bfloat16)
    numerator = jnp.einsum(
        "tgjr,rgd->tgjd",
        weights,
        cache_values.reshape(-1, kv_heads, HD),
        preferred_element_type=jnp.float32,
    )
    denominator = jnp.sum(weights, axis=3, dtype=jnp.float32, keepdims=True)
    shares = jnp.concatenate([numerator, peak, denominator], axis=3)
    shares = shares.reshape(-1, rows_here, heads, HD + 2)
    shares = lax.all_to_all(shares, "blk", 0, 0)
    shares = lax.all_gather(shares, "sub", axis=0, tiled=True)
    peaks = shares[..., HD]
    peak = jnp.max(peaks, axis=0)
    scales = jnp.exp(peaks - peak)
    numerator = jnp.sum(shares[..., :HD] * scales[..., None], axis=0)
    denominator = jnp.sum(shares[..., HD + 1] * scales, axis=0)
    attended = (numerator / denominator[..., None]).astype(jnp.bfloat16)
    return (attended.reshape(rows_here, columns), peak)


def solution(mesh):
    placed = (
        P("blk", "kv"),
        P(("blk", "sub"), "kv"),
        P(("blk", "sub"), "kv"),
        P(("blk", "sub")),
        P(),
    )
    blk, sub = mesh.shape["blk"], mesh.shape["sub"]
    is_direct = (blk, sub) == (4, 2) and mesh.size <= 32

    def on_device(queries, *cache):
        if is_direct and queries.shape[0] == 1:
            return direct((blk, sub), queries, *cache)
        return grouped(queries, *cache)

    return jax.shard_map(
        on_device,
        mesh=mesh,
        in_specs=placed,
        out_specs=(P("blk", "kv"), P("blk", "kv")),
        check_vma=False,
    )
```

```python
import functools
import math

import jax
import jax.numpy as jnp
from jax import lax
from jax.experimental import pallas as pl
from jax.experimental.pallas import tpu as pltpu
from jax.sharding import PartitionSpec as P


HD = 128
HIDDEN = -1e30
DIGIT_ROWS = 16
VMEM_BYTES = 8 * 1024 * 1024


def whole(shape, dtype):
    return jax.ShapeDtypeStruct(shape, dtype)


def params():
    return pltpu.CompilerParams(vmem_limit_bytes=VMEM_BYTES)


def in_vmem(n):
    return [pl.BlockSpec(memory_space=pltpu.VMEM)] * n


def cost(flops):
    return pl.CostEstimate(flops=flops, bytes_accessed=flops // 8, transcendentals=0)


def share_of(query, blocks, shown_rows):
    heads = query.shape[1] // HD
    kv_heads = blocks[0][0].shape[1] // HD
    group = heads // kv_heads
    rows = jnp.concatenate([query[:, i * HD : (i + 1) * HD] for i in range(heads)], axis=0)
    kv_of = lax.broadcasted_iota(jnp.int32, (heads, HD), 0) // group
    lane = lax.broadcasted_iota(jnp.int32, (heads, HD), 1)
    spread = jnp.concatenate(
        [jnp.where(kv_of == j, rows, jnp.zeros_like(rows)) for j in range(kv_heads)], axis=1
    )
    scores = [
        jnp.where(
            shown,
            lax.dot_general(
                spread, keys, (((1,), (1,)), ((), ())), preferred_element_type=jnp.float32
            )
            * (1.0 / math.sqrt(HD)),
            HIDDEN,
        )
        for (keys, _), shown in zip(blocks, shown_rows, strict=True)
    ]
    peak = functools.reduce(jnp.maximum, [jnp.max(s, axis=1, keepdims=True) for s in scores])
    weights = [
        jnp.where(shown, jnp.exp(s - peak), 0.0).astype(jnp.bfloat16)
        for s, shown in zip(scores, shown_rows, strict=True)
    ]
    denominator = sum(jnp.sum(w.astype(jnp.float32), axis=1, keepdims=True) for w in weights)
    wide = sum(
        jnp.dot(w, values, preferred_element_type=jnp.float32)
        for w, (_, values) in zip(weights, blocks, strict=True)
    )
    numerator = wide[:, :HD]
    for j in range(1, kv_heads):
        numerator = jnp.where(kv_of == j, wide[:, j * HD : (j + 1) * HD], numerator)
    return jnp.concatenate([numerator, jnp.where(lane < HD // 2, peak, denominator)], axis=1)


def tokens_kernel(owners, tokens_ref):
    for i, owner in enumerate(owners):
        at = owner(lax.axis_index("blk"))
        tokens_ref[i : i + 1] = jnp.full((1, tokens_ref.shape[1]), at, jnp.int32)


def clock_kernel(start_ref, tokens_ref, clock_ref):
    clock_ref[...] = tokens_ref[...] + start_ref[0]


def pack_kernel(keys_ref, values_ref, places_ref, packed_ref):
    rows, columns = keys_ref.shape
    packed_ref[:rows] = keys_ref[...]
    packed_ref[rows : 2 * rows] = values_ref[...]
    places = places_ref[...].reshape(1, rows)
    digit = lax.broadcasted_iota(jnp.int32, (DIGIT_ROWS, rows), 0)
    digits = jnp.where(digit == 0, places >> 8, jnp.where(digit == 1, places & 255, 0))
    packed_ref[2 * rows :, :rows] = digits.astype(jnp.float32).astype(jnp.bfloat16)
    packed_ref[2 * rows :, rows:] = jnp.zeros((DIGIT_ROWS, columns - rows), jnp.bfloat16)


def share_kernel(row, clock_ref, query_ref, *refs):
    clock = clock_ref[row : row + 1].astype(jnp.float32)
    rows = (refs[0].shape[0] - DIGIT_ROWS) // 2
    blocks, shown = [], []
    for ref in refs[:-1]:
        blocks.append((ref[:rows], ref[rows : 2 * rows]))
        digits = ref[2 * rows :, :rows].astype(jnp.float32)
        shown.append(digits[:1] * 256.0 + digits[1:2] <= clock)
    refs[-1][...] = share_of(query_ref[...], blocks, shown)


def combine_kernel(*refs):
    shares = [r[...] for r in refs[:-2]]
    out_ref, peak_ref = refs[-2:]
    heads = shares[0].shape[0]
    peaks = [s[:, HD : HD + 1] for s in shares]
    peak = functools.reduce(jnp.maximum, peaks)
    scales = [jnp.exp(p - peak) for p in peaks]
    numerator = sum(s[:, :HD] * c for s, c in zip(shares, scales, strict=True))
    denominator = sum(
        s[:, HD + HD // 2 : HD + HD // 2 + 1] * c for s, c in zip(shares, scales, strict=True)
    )
    out = (numerator / denominator).astype(jnp.bfloat16)
    for h in range(heads):
        out_ref[:, h * HD : (h + 1) * HD] = out[h : h + 1]
    row = lax.broadcasted_iota(jnp.int32, (heads, heads), 0)
    column = lax.broadcasted_iota(jnp.int32, (heads, heads), 1)
    peak_ref[...] = jnp.sum(
        jnp.where(row == column, peak, 0.0), axis=0, keepdims=True
    )


def combine(shares, columns):
    heads = shares[0].shape[0]
    return pl.pallas_call(
        combine_kernel,
        out_shape=(whole((1, columns), jnp.bfloat16), whole((1, heads), jnp.float32)),
        in_specs=in_vmem(len(shares)),
        out_specs=tuple(in_vmem(2)),
        compiler_params=params(),
        cost_estimate=cost(1 << 16),
        name="combine",
    )(*shares)


def direct(sizes, queries, cache_keys, cache_values, cache_places, span_start):
    blk, sub = sizes
    columns = queries.shape[1]
    heads = columns // HD
    row_count = cache_keys.shape[0]
    both = ("blk", "sub")

    def swap(value, flip_block, flip_sub):
        pairs = [
            (b * sub + s, (b ^ flip_block) * sub + (s ^ flip_sub))
            for b in range(blk)
            for s in range(sub)
        ]
        return lax.ppermute(value, both, pairs)

    def share(row, query):
        return pl.pallas_call(
            functools.partial(share_kernel, row),
            out_shape=whole((heads, 2 * HD), jnp.float32),
            in_specs=in_vmem(4),
            out_specs=in_vmem(1)[0],
            compiler_params=params(),
            cost_estimate=cost(1 << 22),
        )(clock, query, mine, theirs)

    other_query = swap(queries, 3, 0)
    mine = pl.pallas_call(
        pack_kernel,
        out_shape=whole((2 * row_count + DIGIT_ROWS, cache_keys.shape[1]), jnp.bfloat16),
        in_specs=in_vmem(3),
        out_specs=in_vmem(1)[0],
        compiler_params=params(),
        cost_estimate=cost(1 << 12),
        name="pack",
    )(cache_keys, cache_values, cache_places)
    theirs = swap(mine, 1, 0)
    tokens = pl.pallas_call(
        functools.partial(tokens_kernel, (lambda b: b, lambda b: b ^ 3)),
        out_shape=whole((2, row_count), jnp.int32),
        out_specs=in_vmem(1)[0],
        compiler_params=params(),
        cost_estimate=pl.CostEstimate(
            flops=1 << 27, bytes_accessed=4096, transcendentals=0
        ),
        name="tokens",
    )()
    clock = pl.pallas_call(
        clock_kernel,
        out_shape=whole((2, row_count), jnp.int32),
        in_specs=[pl.BlockSpec(memory_space=pltpu.SMEM)] + in_vmem(1),
        out_specs=in_vmem(1)[0],
        compiler_params=params(),
        cost_estimate=cost(1 << 12),
        name="clock",
    )(span_start, tokens)
    own_share = share(0, queries)
    across = swap(own_share, 0, 1)
    other_share = share(1, other_query)
    shares = [own_share, across, swap(other_share, 3, 1), swap(other_share, 3, 0)]
    return combine(shares, columns)


def grouped(queries, cache_keys, cache_values, cache_places, span_start):
    columns = queries.shape[1]
    heads = columns // HD
    kv_heads = cache_keys.shape[1] // HD
    rows_here = queries.shape[0]
    gathered = lax.all_gather(queries, "blk", axis=0, tiled=True)
    count = gathered.shape[0]
    at = span_start[0] + jnp.arange(count, dtype=jnp.int32)
    scores = jnp.einsum(
        "tgjd,rgd->tgjr",
        gathered.reshape(count, kv_heads, heads // kv_heads, HD),
        cache_keys.reshape(-1, kv_heads, HD),
        preferred_element_type=jnp.float32,
    ) * (1.0 / math.sqrt(HD))
    shown = (cache_places[None, :] <= at[:, None])[:, None, None, :]
    scores = jnp.where(shown, scores, HIDDEN)
    peak = jnp.max(scores, axis=3, keepdims=True)
    weights = jnp.where(shown, jnp.exp(scores - peak), 0.0).astype(jnp.bfloat16)
    numerator = jnp.einsum(
        "tgjr,rgd->tgjd",
        weights,
        cache_values.reshape(-1, kv_heads, HD),
        preferred_element_type=jnp.float32,
    )
    denominator = jnp.sum(weights, axis=3, dtype=jnp.float32, keepdims=True)
    shares = jnp.concatenate([numerator, peak, denominator], axis=3)
    shares = shares.reshape(-1, rows_here, heads, HD + 2)
    shares = lax.all_to_all(shares, "blk", 0, 0)
    shares = lax.all_gather(shares, "sub", axis=0, tiled=True)
    peaks = shares[..., HD]
    peak = jnp.max(peaks, axis=0)
    scales = jnp.exp(peaks - peak)
    numerator = jnp.sum(shares[..., :HD] * scales[..., None], axis=0)
    denominator = jnp.sum(shares[..., HD + 1] * scales, axis=0)
    attended = (numerator / denominator[..., None]).astype(jnp.bfloat16)
    return (attended.reshape(rows_here, columns), peak)


def solution(mesh):
    placed = (
        P("blk", "kv"),
        P(("blk", "sub"), "kv"),
        P(("blk", "sub"), "kv"),
        P(("blk", "sub")),
        P(),
    )
    blk, sub = mesh.shape["blk"], mesh.shape["sub"]
    is_direct = (blk, sub) == (4, 2) and mesh.size <= 32

    def on_device(queries, *cache):
        if is_direct and queries.shape[0] == 1:
            return direct((blk, sub), queries, *cache)
        return grouped(queries, *cache)

    return jax.shard_map(
        on_device,
        mesh=mesh,
        in_specs=placed,
        out_specs=(P("blk", "kv"), P("blk", "kv")),
        check_vma=False,
    )
```

```python
import functools
import math

import jax
import jax.numpy as jnp
from jax import lax
from jax.experimental import pallas as pl
from jax.experimental.pallas import tpu as pltpu
from jax.sharding import PartitionSpec as P


HD = 128
HIDDEN = -1e30
DIGIT_ROWS = 16
VMEM_BYTES = 8 * 1024 * 1024


def whole(shape, dtype):
    return jax.ShapeDtypeStruct(shape, dtype)


def params():
    return pltpu.CompilerParams(vmem_limit_bytes=VMEM_BYTES)


def in_vmem(n):
    return [pl.BlockSpec(memory_space=pltpu.VMEM)] * n


def cost(flops):
    return pl.CostEstimate(flops=flops, bytes_accessed=flops // 8, transcendentals=0)


def share_of(query, blocks, shown_rows):
    heads = query.shape[1] // HD
    kv_heads = blocks[0][0].shape[1] // HD
    group = heads // kv_heads
    rows = jnp.concatenate([query[:, i * HD : (i + 1) * HD] for i in range(heads)], axis=0)
    kv_of = lax.broadcasted_iota(jnp.int32, (heads, HD), 0) // group
    lane = lax.broadcasted_iota(jnp.int32, (heads, HD), 1)
    spread = jnp.concatenate(
        [jnp.where(kv_of == j, rows, jnp.zeros_like(rows)) for j in range(kv_heads)], axis=1
    )
    scores = [
        jnp.where(
            shown,
            lax.dot_general(
                spread, keys, (((1,), (1,)), ((), ())), preferred_element_type=jnp.float32
            )
            * (1.0 / math.sqrt(HD)),
            HIDDEN,
        )
        for (keys, _), shown in zip(blocks, shown_rows, strict=True)
    ]
    peak = functools.reduce(jnp.maximum, [jnp.max(s, axis=1, keepdims=True) for s in scores])
    weights = [
        jnp.where(shown, jnp.exp(s - peak), 0.0).astype(jnp.bfloat16)
        for s, shown in zip(scores, shown_rows, strict=True)
    ]
    denominator = sum(jnp.sum(w.astype(jnp.float32), axis=1, keepdims=True) for w in weights)
    wide = sum(
        jnp.dot(w, values, preferred_element_type=jnp.float32)
        for w, (_, values) in zip(weights, blocks, strict=True)
    )
    numerator = wide[:, :HD]
    for j in range(1, kv_heads):
        numerator = jnp.where(kv_of == j, wide[:, j * HD : (j + 1) * HD], numerator)
    return jnp.concatenate([numerator, jnp.where(lane < HD // 2, peak, denominator)], axis=1)


def tokens_kernel(owners, tokens_ref):
    for i, owner in enumerate(owners):
        at = owner(lax.axis_index("blk"))
        tokens_ref[i : i + 1] = jnp.full((1, tokens_ref.shape[1]), at, jnp.int32)


def clock_kernel(start_ref, tokens_ref, clock_ref):
    clock_ref[...] = tokens_ref[...] + start_ref[0]


def pack_kernel(keys_ref, values_ref, places_ref, packed_ref):
    rows, columns = keys_ref.shape
    packed_ref[:rows] = keys_ref[...]
    packed_ref[rows : 2 * rows] = values_ref[...]
    places = places_ref[...].reshape(1, rows)
    digit = lax.broadcasted_iota(jnp.int32, (DIGIT_ROWS, rows), 0)
    digits = jnp.where(digit == 0, places >> 8, jnp.where(digit == 1, places & 255, 0))
    packed_ref[2 * rows :, :rows] = digits.astype(jnp.float32).astype(jnp.bfloat16)
    packed_ref[2 * rows :, rows:] = jnp.zeros((DIGIT_ROWS, columns - rows), jnp.bfloat16)


def share_kernel(row, clock_ref, query_ref, *refs):
    clock = clock_ref[row : row + 1].astype(jnp.float32)
    rows = (refs[0].shape[0] - DIGIT_ROWS) // 2
    blocks, shown = [], []
    for ref in refs[:-1]:
        blocks.append((ref[:rows], ref[rows : 2 * rows]))
        digits = ref[2 * rows :, :rows].astype(jnp.float32)
        shown.append(digits[:1] * 256.0 + digits[1:2] <= clock)
    refs[-1][...] = share_of(query_ref[...], blocks, shown)


def combine_kernel(*refs):
    shares = [r[...] for r in refs[:-2]]
    out_ref, peak_ref = refs[-2:]
    heads = shares[0].shape[0]
    left = lax.broadcasted_iota(jnp.int32, (heads, HD), 1) < HD // 2
    stats = [s[:, HD:] for s in shares]
    turned = [pltpu.roll(s, HD // 2, 1) for s in stats]
    peaks = [jnp.where(left, s, t) for s, t in zip(stats, turned, strict=True)]
    peak = functools.reduce(jnp.maximum, peaks)
    scales = [jnp.exp(p - peak) for p in peaks]
    numerator = sum(s[:, :HD] * c for s, c in zip(shares, scales, strict=True))
    denominator = sum(
        jnp.where(left, t, s) * c for s, t, c in zip(stats, turned, scales, strict=True)
    )
    out = (numerator / denominator).astype(jnp.bfloat16)
    for h in range(heads):
        out_ref[:, h * HD : (h + 1) * HD] = out[h : h + 1]
    row = lax.broadcasted_iota(jnp.int32, (heads, heads), 0)
    column = lax.broadcasted_iota(jnp.int32, (heads, heads), 1)
    peak_ref[...] = jnp.sum(
        jnp.where(row == column, peak[:, :heads], 0.0), axis=0, keepdims=True
    )


def combine(shares, columns):
    heads = shares[0].shape[0]
    return pl.pallas_call(
        combine_kernel,
        out_shape=(whole((1, columns), jnp.bfloat16), whole((1, heads), jnp.float32)),
        in_specs=in_vmem(len(shares)),
        out_specs=tuple(in_vmem(2)),
        compiler_params=params(),
        cost_estimate=cost(1 << 16),
        name="combine",
    )(*shares)


def direct(sizes, queries, cache_keys, cache_values, cache_places, span_start):
    blk, sub = sizes
    columns = queries.shape[1]
    heads = columns // HD
    row_count = cache_keys.shape[0]
    both = ("blk", "sub")

    def swap(value, flip_block, flip_sub):
        pairs = [
            (b * sub + s, (b ^ flip_block) * sub + (s ^ flip_sub))
            for b in range(blk)
            for s in range(sub)
        ]
        return lax.ppermute(value, both, pairs)

    def share(row, query):
        return pl.pallas_call(
            functools.partial(share_kernel, row),
            out_shape=whole((heads, 2 * HD), jnp.float32),
            in_specs=in_vmem(4),
            out_specs=in_vmem(1)[0],
            compiler_params=params(),
            cost_estimate=cost(1 << 22),
        )(clock, query, mine, theirs)

    other_query = swap(queries, 3, 0)
    mine = pl.pallas_call(
        pack_kernel,
        out_shape=whole((2 * row_count + DIGIT_ROWS, cache_keys.shape[1]), jnp.bfloat16),
        in_specs=in_vmem(3),
        out_specs=in_vmem(1)[0],
        compiler_params=params(),
        cost_estimate=cost(1 << 12),
        name="pack",
    )(cache_keys, cache_values, cache_places)
    theirs = swap(mine, 1, 0)
    tokens = pl.pallas_call(
        functools.partial(tokens_kernel, (lambda b: b, lambda b: b ^ 3)),
        out_shape=whole((2, row_count), jnp.int32),
        out_specs=in_vmem(1)[0],
        compiler_params=params(),
        cost_estimate=pl.CostEstimate(
            flops=1 << 27, bytes_accessed=4096, transcendentals=0
        ),
        name="tokens",
    )()
    clock = pl.pallas_call(
        clock_kernel,
        out_shape=whole((2, row_count), jnp.int32),
        in_specs=[pl.BlockSpec(memory_space=pltpu.SMEM)] + in_vmem(1),
        out_specs=in_vmem(1)[0],
        compiler_params=params(),
        cost_estimate=cost(1 << 12),
        name="clock",
    )(span_start, tokens)
    own_share = share(0, queries)
    across = swap(own_share, 0, 1)
    other_share = share(1, other_query)
    shares = [own_share, across, swap(other_share, 3, 1), swap(other_share, 3, 0)]
    return combine(shares, columns)


def grouped(queries, cache_keys, cache_values, cache_places, span_start):
    columns = queries.shape[1]
    heads = columns // HD
    kv_heads = cache_keys.shape[1] // HD
    rows_here = queries.shape[0]
    gathered = lax.all_gather(queries, "blk", axis=0, tiled=True)
    count = gathered.shape[0]
    at = span_start[0] + jnp.arange(count, dtype=jnp.int32)
    scores = jnp.einsum(
        "tgjd,rgd->tgjr",
        gathered.reshape(count, kv_heads, heads // kv_heads, HD),
        cache_keys.reshape(-1, kv_heads, HD),
        preferred_element_type=jnp.float32,
    ) * (1.0 / math.sqrt(HD))
    shown = (cache_places[None, :] <= at[:, None])[:, None, None, :]
    scores = jnp.where(shown, scores, HIDDEN)
    peak = jnp.max(scores, axis=3, keepdims=True)
    weights = jnp.where(shown, jnp.exp(scores - peak), 0.0).astype(jnp.bfloat16)
    numerator = jnp.einsum(
        "tgjr,rgd->tgjd",
        weights,
        cache_values.reshape(-1, kv_heads, HD),
        preferred_element_type=jnp.float32,
    )
    denominator = jnp.sum(weights, axis=3, dtype=jnp.float32, keepdims=True)
    shares = jnp.concatenate([numerator, peak, denominator], axis=3)
    shares = shares.reshape(-1, rows_here, heads, HD + 2)
    shares = lax.all_to_all(shares, "blk", 0, 0)
    shares = lax.all_gather(shares, "sub", axis=0, tiled=True)
    peaks = shares[..., HD]
    peak = jnp.max(peaks, axis=0)
    scales = jnp.exp(peaks - peak)
    numerator = jnp.sum(shares[..., :HD] * scales[..., None], axis=0)
    denominator = jnp.sum(shares[..., HD + 1] * scales, axis=0)
    attended = (numerator / denominator[..., None]).astype(jnp.bfloat16)
    return (attended.reshape(rows_here, columns), peak)


def solution(mesh):
    placed = (
        P("blk", "kv"),
        P(("blk", "sub"), "kv"),
        P(("blk", "sub"), "kv"),
        P(("blk", "sub")),
        P(),
    )
    blk, sub = mesh.shape["blk"], mesh.shape["sub"]
    is_direct = (blk, sub) == (4, 2) and mesh.size <= 32

    def on_device(queries, *cache):
        if is_direct and queries.shape[0] == 1:
            return direct((blk, sub), queries, *cache)
        return grouped(queries, *cache)

    return jax.shard_map(
        on_device,
        mesh=mesh,
        in_specs=placed,
        out_specs=(P("blk", "kv"), P("blk", "kv")),
        check_vma=False,
    )
```

```python
import functools
import math

import jax
import jax.numpy as jnp
from jax import lax
from jax.experimental import pallas as pl
from jax.experimental.pallas import tpu as pltpu
from jax.sharding import PartitionSpec as P


HD = 128
HIDDEN = -1e30
DIGIT_ROWS = 16
VMEM_BYTES = 8 * 1024 * 1024


def whole(shape, dtype):
    return jax.ShapeDtypeStruct(shape, dtype)


def params():
    return pltpu.CompilerParams(vmem_limit_bytes=VMEM_BYTES)


def in_vmem(n):
    return [pl.BlockSpec(memory_space=pltpu.VMEM)] * n


def cost(flops):
    return pl.CostEstimate(flops=flops, bytes_accessed=flops // 8, transcendentals=0)


def share_of(query, blocks, shown_rows):
    heads = query.shape[1] // HD
    kv_heads = blocks[0][0].shape[1] // HD
    group = heads // kv_heads
    rows = jnp.concatenate([query[:, i * HD : (i + 1) * HD] for i in range(heads)], axis=0)
    kv_of = lax.broadcasted_iota(jnp.int32, (heads, HD), 0) // group
    lane = lax.broadcasted_iota(jnp.int32, (heads, HD), 1)
    spread = jnp.concatenate(
        [jnp.where(kv_of == j, rows, jnp.zeros_like(rows)) for j in range(kv_heads)], axis=1
    )
    scores = [
        jnp.where(
            shown,
            lax.dot_general(
                spread, keys, (((1,), (1,)), ((), ())), preferred_element_type=jnp.float32
            )
            * (1.0 / math.sqrt(HD)),
            HIDDEN,
        )
        for (keys, _), shown in zip(blocks, shown_rows, strict=True)
    ]
    peak = functools.reduce(jnp.maximum, [jnp.max(s, axis=1, keepdims=True) for s in scores])
    weights = [
        jnp.where(shown, jnp.exp(s - peak), 0.0).astype(jnp.bfloat16)
        for s, shown in zip(scores, shown_rows, strict=True)
    ]
    denominator = sum(jnp.sum(w.astype(jnp.float32), axis=1, keepdims=True) for w in weights)
    wide = sum(
        jnp.dot(w, values, preferred_element_type=jnp.float32)
        for w, (_, values) in zip(weights, blocks, strict=True)
    )
    numerator = wide[:, :HD]
    for j in range(1, kv_heads):
        numerator = jnp.where(kv_of == j, wide[:, j * HD : (j + 1) * HD], numerator)
    return jnp.concatenate([numerator, jnp.where(lane < HD // 2, peak, denominator)], axis=1)


def tokens_kernel(owners, tokens_ref):
    for i, owner in enumerate(owners):
        at = owner(lax.axis_index("blk"))
        tokens_ref[i : i + 1] = jnp.full((1, tokens_ref.shape[1]), at, jnp.int32)


def clock_kernel(start_ref, tokens_ref, clock_ref):
    clock_ref[...] = tokens_ref[...] + start_ref[0]


def pack_kernel(keys_ref, values_ref, places_ref, packed_ref):
    rows, columns = keys_ref.shape
    packed_ref[:rows] = keys_ref[...]
    packed_ref[rows : 2 * rows] = values_ref[...]
    places = places_ref[...].reshape(1, rows)
    digit = lax.broadcasted_iota(jnp.int32, (DIGIT_ROWS, rows), 0)
    digits = jnp.where(digit == 0, places >> 8, jnp.where(digit == 1, places & 255, 0))
    packed_ref[2 * rows :, :rows] = digits.astype(jnp.float32).astype(jnp.bfloat16)
    packed_ref[2 * rows :, rows:] = jnp.zeros((DIGIT_ROWS, columns - rows), jnp.bfloat16)


def share_kernel(row, clock_ref, query_ref, *refs):
    clock = clock_ref[row : row + 1].astype(jnp.float32)
    rows = (refs[0].shape[0] - DIGIT_ROWS) // 2
    blocks, shown = [], []
    for ref in refs[:-1]:
        blocks.append((ref[:rows], ref[rows : 2 * rows]))
        digits = ref[2 * rows :, :rows].astype(jnp.float32)
        shown.append(digits[:1] * 256.0 + digits[1:2] <= clock)
    refs[-1][...] = share_of(query_ref[...], blocks, shown)


def merged(shares):
    left = lax.broadcasted_iota(jnp.int32, (shares[0].shape[0], HD), 1) < HD // 2
    stats = [s[:, HD:] for s in shares]
    turned = [pltpu.roll(s, HD // 2, 1) for s in stats]
    peaks = [jnp.where(left, s, t) for s, t in zip(stats, turned, strict=True)]
    peak = functools.reduce(jnp.maximum, peaks)
    scales = [jnp.exp(p - peak) for p in peaks]
    numerator = sum(s[:, :HD] * c for s, c in zip(shares, scales, strict=True))
    denominator = sum(
        jnp.where(left, t, s) * c for s, t, c in zip(stats, turned, scales, strict=True)
    )
    return numerator, peak, denominator, left


def merge_kernel(*refs):
    numerator, peak, denominator, left = merged([r[...] for r in refs[:-1]])
    refs[-1][...] = jnp.concatenate([numerator, jnp.where(left, peak, denominator)], axis=1)


def combine_kernel(*refs):
    shares = [r[...] for r in refs[:-2]]
    out_ref, peak_ref = refs[-2:]
    heads = shares[0].shape[0]
    numerator, peak, denominator, _ = merged(shares)
    out = (numerator / denominator).astype(jnp.bfloat16)
    for h in range(heads):
        out_ref[:, h * HD : (h + 1) * HD] = out[h : h + 1]
    row = lax.broadcasted_iota(jnp.int32, (heads, heads), 0)
    column = lax.broadcasted_iota(jnp.int32, (heads, heads), 1)
    peak_ref[...] = jnp.sum(
        jnp.where(row == column, peak[:, :heads], 0.0), axis=0, keepdims=True
    )


def combine(shares, columns):
    heads = shares[0].shape[0]
    return pl.pallas_call(
        combine_kernel,
        out_shape=(whole((1, columns), jnp.bfloat16), whole((1, heads), jnp.float32)),
        in_specs=in_vmem(len(shares)),
        out_specs=tuple(in_vmem(2)),
        compiler_params=params(),
        cost_estimate=cost(1 << 16),
        name="combine",
    )(*shares)


def direct(sizes, queries, cache_keys, cache_values, cache_places, span_start):
    blk, sub = sizes
    columns = queries.shape[1]
    heads = columns // HD
    row_count = cache_keys.shape[0]
    both = ("blk", "sub")

    def swap(value, flip_block, flip_sub):
        pairs = [
            (b * sub + s, (b ^ flip_block) * sub + (s ^ flip_sub))
            for b in range(blk)
            for s in range(sub)
        ]
        return lax.ppermute(value, both, pairs)

    def share(row, query):
        return pl.pallas_call(
            functools.partial(share_kernel, row),
            out_shape=whole((heads, 2 * HD), jnp.float32),
            in_specs=in_vmem(4),
            out_specs=in_vmem(1)[0],
            compiler_params=params(),
            cost_estimate=cost(1 << 22),
        )(clock, query, mine, theirs)

    other_query = swap(queries, 3, 0)
    mine = pl.pallas_call(
        pack_kernel,
        out_shape=whole((2 * row_count + DIGIT_ROWS, cache_keys.shape[1]), jnp.bfloat16),
        in_specs=in_vmem(3),
        out_specs=in_vmem(1)[0],
        compiler_params=params(),
        cost_estimate=cost(1 << 12),
        name="pack",
    )(cache_keys, cache_values, cache_places)
    theirs = swap(mine, 1, 0)
    tokens = pl.pallas_call(
        functools.partial(tokens_kernel, (lambda b: b, lambda b: b ^ 3)),
        out_shape=whole((2, row_count), jnp.int32),
        out_specs=in_vmem(1)[0],
        compiler_params=params(),
        cost_estimate=pl.CostEstimate(
            flops=1 << 27, bytes_accessed=4096, transcendentals=0
        ),
        name="tokens",
    )()
    clock = pl.pallas_call(
        clock_kernel,
        out_shape=whole((2, row_count), jnp.int32),
        in_specs=[pl.BlockSpec(memory_space=pltpu.SMEM)] + in_vmem(1),
        out_specs=in_vmem(1)[0],
        compiler_params=params(),
        cost_estimate=cost(1 << 12),
        name="clock",
    )(span_start, tokens)
    own_share = share(0, queries)
    across = swap(own_share, 0, 1)
    other_share = share(1, other_query)
    corner = swap(other_share, 3, 1)
    near = swap(other_share, 3, 0)
    gathered = pl.pallas_call(
        merge_kernel,
        out_shape=whole((heads, 2 * HD), jnp.float32),
        in_specs=in_vmem(3),
        out_specs=in_vmem(1)[0],
        compiler_params=params(),
        cost_estimate=cost(1 << 16),
        name="merge",
    )(own_share, across, corner)
    return combine([gathered, near], columns)


def grouped(queries, cache_keys, cache_values, cache_places, span_start):
    columns = queries.shape[1]
    heads = columns // HD
    kv_heads = cache_keys.shape[1] // HD
    rows_here = queries.shape[0]
    gathered = lax.all_gather(queries, "blk", axis=0, tiled=True)
    count = gathered.shape[0]
    at = span_start[0] + jnp.arange(count, dtype=jnp.int32)
    scores = jnp.einsum(
        "tgjd,rgd->tgjr",
        gathered.reshape(count, kv_heads, heads // kv_heads, HD),
        cache_keys.reshape(-1, kv_heads, HD),
        preferred_element_type=jnp.float32,
    ) * (1.0 / math.sqrt(HD))
    shown = (cache_places[None, :] <= at[:, None])[:, None, None, :]
    scores = jnp.where(shown, scores, HIDDEN)
    peak = jnp.max(scores, axis=3, keepdims=True)
    weights = jnp.where(shown, jnp.exp(scores - peak), 0.0).astype(jnp.bfloat16)
    numerator = jnp.einsum(
        "tgjr,rgd->tgjd",
        weights,
        cache_values.reshape(-1, kv_heads, HD),
        preferred_element_type=jnp.float32,
    )
    denominator = jnp.sum(weights, axis=3, dtype=jnp.float32, keepdims=True)
    shares = jnp.concatenate([numerator, peak, denominator], axis=3)
    shares = shares.reshape(-1, rows_here, heads, HD + 2)
    shares = lax.all_to_all(shares, "blk", 0, 0)
    shares = lax.all_gather(shares, "sub", axis=0, tiled=True)
    peaks = shares[..., HD]
    peak = jnp.max(peaks, axis=0)
    scales = jnp.exp(peaks - peak)
    numerator = jnp.sum(shares[..., :HD] * scales[..., None], axis=0)
    denominator = jnp.sum(shares[..., HD + 1] * scales, axis=0)
    attended = (numerator / denominator[..., None]).astype(jnp.bfloat16)
    return (attended.reshape(rows_here, columns), peak)


def solution(mesh):
    placed = (
        P("blk", "kv"),
        P(("blk", "sub"), "kv"),
        P(("blk", "sub"), "kv"),
        P(("blk", "sub")),
        P(),
    )
    blk, sub = mesh.shape["blk"], mesh.shape["sub"]
    is_direct = (blk, sub) == (4, 2) and mesh.size <= 32

    def on_device(queries, *cache):
        if is_direct and queries.shape[0] == 1:
            return direct((blk, sub), queries, *cache)
        return grouped(queries, *cache)

    return jax.shard_map(
        on_device,
        mesh=mesh,
        in_specs=placed,
        out_specs=(P("blk", "kv"), P("blk", "kv")),
        check_vma=False,
    )
```
